32 devices in a mesh: band: 8 (over z, y), dom: 4 (over x, core).
Axes of the slice: x: 2, y: 2, z: 4, core: 2. Of those that a mesh axis runs over, the one named last changes fastest.
Arguments:
- wavefunctions: float32 [1024, 16, 16, 128], P('band', 'dom'), may hold values from -6 to 6
- potential: float32 [16, 16, 128], P('dom'), may hold values from -40 to 40
- projectors: float32 [16, 18, 4, 16, 128], P('dom'), may hold values from -0.0625 to 0.0625
- hamiltonian_correction: float32 [16, 18, 18], P('dom'), may hold values from -0.078125 to 0.078125
- delta_s: float32 [16, 18, 18], P('dom'), may hold values from -0.078125 to 0.078125
- projector_count: int32 [16], P('dom'), may hold values from 1 to 18
Outputs:
- ham: float32 [1024, 1024], P('band')
- correlation: float32 [1024, 1024], P('band')
The draws below stay inside these ranges and needn't reach their ends.
All inputs are finite; a program needn't handle non-finite values.
Results may differ from the reference program's by a relative error of at most 0.00007.
Values sent between devices are 32-bit elements; how exact they have to be, the bound alone decides.
A program may use at most 192 MiB of HBM per device.

```python
import jax
import jax.numpy as jnp
from jax import lax

BANDS = 1024
NPROJ = 18
A_DEV = 4
CX = 4
NY = 16
NZ = 128
NX = 16
ATOMS = 16
N_DOM = 4


def place_ends(entries, rng, least, largest):
    extent = entries.shape
    index_at = [jax.random.randint(jax.random.fold_in(rng, axis), (), 0, extent[axis]) for axis in range(len(extent))]
    entries = entries.at[tuple(index_at)].set(least)
    longest = extent.index(max(extent))
    index_at[longest] = (index_at[longest] + 1) % extent[longest]
    return entries.at[tuple(index_at)].set(largest)


def block_levels(rng, dims, pieces, least, top_value):
    gain = 1.0
    for axis_at, parts in pieces:
        heights = jax.random.uniform(jax.random.fold_in(jax.random.fold_in(rng, 6), axis_at), (parts,), jnp.float32, least / len(pieces), top_value / len(pieces))
        gain = gain * jnp.repeat(jnp.exp(heights), dims[axis_at] // parts).reshape((-1,) + (1,) * (len(dims) - 1 - axis_at))
    return gain


def centred(stream_key, shape, deviation, reach, cuts=(), kind=jnp.bfloat16):
    result = deviation * jax.random.normal(stream_key, shape, jnp.float32)
    if cuts:
        result = result * block_levels(stream_key, shape, cuts, -0.22, 0.18)
    return jnp.clip(result, -reach, reach).astype(kind)


def setup_inputs(seed: int = 0) -> dict:
    arg_keys = jax.random.split(jax.random.key(seed), 7)
    return {
        "wavefunctions": centred(arg_keys[0], (BANDS, NX, NY, NZ), 1.0, 6.0, ((0, 8), (1, 4)), jnp.float32),
        "potential": jnp.clip(jax.random.uniform(arg_keys[1], (NX, NY, NZ), jnp.float32, -40.0, 40.0) * block_levels(arg_keys[1], (NX, NY, NZ), ((0, 4),), -0.4, 0.0), -40.0, 40.0),
        "projectors": centred(arg_keys[2], (ATOMS, NPROJ, CX, NY, NZ), (CX * NY * NZ) ** -0.5, 0.0625, ((0, 4),), jnp.float32),
        "hamiltonian_correction": centred(arg_keys[3], (ATOMS, NPROJ, NPROJ), (ATOMS * NPROJ * NPROJ) ** -0.5, 0.078125, ((0, 4),), jnp.float32),
        "delta_s": centred(arg_keys[4], (ATOMS, NPROJ, NPROJ), (ATOMS * NPROJ * NPROJ) ** -0.5, 0.078125, ((0, 4),), jnp.float32),
        "projector_count": place_ends(jax.random.randint(arg_keys[5], (ATOMS,), 1, NPROJ + 1), jax.random.fold_in(arg_keys[5], 1), 1, NPROJ).astype(jnp.int32),
    }


def rows_product(left, right):
    return lax.dot_general(left, right, (((1,), (1,)), ((), ())), precision=lax.Precision.HIGHEST, preferred_element_type=jnp.float32)


def reference(wavefunctions, potential, projectors, hamiltonian_correction, delta_s, projector_count):
    bands = wavefunctions.shape[0]
    beside = jnp.roll(wavefunctions, 1, 1) + jnp.roll(wavefunctions, -1, 1)
    beside = beside + jnp.roll(wavefunctions, 1, 2) + jnp.roll(wavefunctions, -1, 2)
    beside = beside + jnp.roll(wavefunctions, 1, 3) + jnp.roll(wavefunctions, -1, 3)
    hpsi = 0.5 * (6.0 * wavefunctions - beside) + potential[None] * wavefunctions
    volume = 1.0 / (NX * NY * NZ)
    local_cells = CX * NY * NZ
    split_psi = wavefunctions.reshape(bands, N_DOM, local_cells)
    split_proj = projectors.reshape(N_DOM, A_DEV * NPROJ, local_cells)
    projector_coefficient = jnp.einsum("bdg,dkg->bdk", split_psi, split_proj, precision=lax.Precision.HIGHEST)
    slot_mask = (jnp.arange(NPROJ, dtype=jnp.int32)[None, :] < projector_count[:, None]).astype(jnp.float32)
    projector_coefficient = projector_coefficient.reshape(bands, ATOMS, NPROJ) * slot_mask[None]
    sym_h = 0.5 * (hamiltonian_correction + jnp.swapaxes(hamiltonian_correction, 1, 2))
    sym_s = 0.5 * (delta_s + jnp.swapaxes(delta_s, 1, 2))
    coupled_h = jnp.einsum("bap,apq->baq", projector_coefficient, sym_h, precision=lax.Precision.HIGHEST).reshape(bands, -1)
    coupled_s = jnp.einsum("bap,apq->baq", projector_coefficient, sym_s, precision=lax.Precision.HIGHEST).reshape(bands, -1)
    coef_flat = projector_coefficient.reshape(bands, -1)
    psi_flat = wavefunctions.reshape(bands, -1)
    hpsi_flat = hpsi.reshape(bands, -1)
    ham = volume * rows_product(hpsi_flat, psi_flat) + rows_product(coupled_h, coef_flat)
    correlation = volume * rows_product(psi_flat, psi_flat) + rows_product(coupled_s, coef_flat)
    return ham, correlation
```

```python
import functools

import jax
import jax.numpy as jnp
from jax import lax
from jax.experimental import pallas as pl
from jax.experimental.pallas import tpu as pltpu
from jax.sharding import PartitionSpec as P

MESH = pl.DeviceIdType.MESH
CONTRACT_LAST = (((1,), (1,)), ((), ()))


def parts(value):
    high = value.astype(jnp.bfloat16)
    low = (value - high.astype(jnp.float32)).astype(jnp.bfloat16)
    return high, low


def gram_kernel(
    lines, doms, cx, ny, chunks,
    psi, pot, proj, sym, out,
    partner, halo, partner_halo, from_left, from_right, lhs_high, lhs_low,
    left_edges, right_edges, coef, coef_below,
    swap_send, swap_recv, halo_send, halo_recv, fwd_send, fwd_recv,
    right_send, right_recv, left_send, left_recv,
    right_edge_send, right_edge_recv, left_edge_send, left_edge_recv,
    coef_send, coef_recv, pair_send, pair_recv,
):
    rows, bands, nz = psi.shape
    half = rows // 2
    step = half // chunks
    hy = ny // 2
    mine = lax.axis_index("band")
    dom = lax.axis_index("dom")
    line = mine // 2
    side = mine % 2
    mirror = lines - 1 - line
    pair = line * 2 + (1 - side)
    upper = jnp.minimum(line + 1, lines - 1) * 2 + side
    lower = jnp.maximum(line - 1, 0) * 2 + side
    dom_next = (dom + 1) % doms
    dom_prev = (dom + doms - 1) % doms
    ends = lines >= 4

    barrier = pltpu.get_barrier_semaphore()
    pl.semaphore_signal(barrier, inc=1, device_id={"band": pair}, device_id_type=MESH)
    pl.semaphore_signal(barrier, inc=1, device_id={"dom": dom_next}, device_id_type=MESH)
    pl.semaphore_signal(barrier, inc=1, device_id={"dom": dom_prev}, device_id_type=MESH)

    @pl.when(line > 0)
    def _():
        pl.semaphore_signal(barrier, inc=1, device_id={"band": lower}, device_id_type=MESH)

    @pl.when(line < lines - 1)
    def _():
        pl.semaphore_signal(barrier, inc=1, device_id={"band": upper}, device_id_type=MESH)

    peers = 3 + jnp.minimum(line, 1) + jnp.minimum(mirror, 1)
    pl.semaphore_wait(barrier, peers)

    def remote(src, dst, send, recv, where):
        return pltpu.make_async_remote_copy(
            src_ref=src, dst_ref=dst, send_sem=send, recv_sem=recv,
            device_id=where, device_id_type=MESH,
        )

    def seg(ref, at):
        return ref.at[pl.ds(at * hy, hy)]

    segs = 2 * cx
    swaps = [
        remote(seg(psi, at), seg(partner, at), swap_send.at[at], swap_recv.at[at], {"band": pair})
        for at in range(segs)
    ]

    def planes_out(src, dst, send, recv):
        return [
            remote(seg(src, h * cx + at), dst.at[edge, h], send.at[edge, h], recv.at[edge, h], {"dom": to})
            for edge, at, to in ((0, cx - 1, dom_next), (1, 0, dom_prev))
            for h in range(2)
        ]

    halos = planes_out(psi, halo, halo_send, halo_recv)
    forwards = planes_out(partner, partner_halo, fwd_send, fwd_recv)
    coef_swap = remote(coef.at[0], coef.at[1], pair_send.at[0], pair_recv.at[0], {"band": pair})

    def coef_hop(dist):
        src = coef.at[0] if dist == 1 else coef_below.at[dist - 2]
        return remote(src, coef_below.at[dist - 1], coef_send.at[dist - 1], coef_recv.at[dist - 1], {"band": upper})

    ways = (
        (0, half, from_left, right_send, right_recv, upper, line, left_edges, right_edge_send, right_edge_recv),
        (half, 0, from_right, left_send, left_recv, lower, mirror, right_edges, left_edge_send, left_edge_recv),
    )

    def hop(way, dist, chunk, extra=False):
        base, other, slots, send, recv, target = way[:6]
        if extra:
            src = psi.at[pl.ds(other + chunk * step, step)]
        elif dist == 1:
            src = psi.at[pl.ds(base + chunk * step, step)]
        else:
            src = slots.at[dist - 2, pl.ds(chunk * step, step)]
        return remote(
            src, slots.at[dist - 1, pl.ds(chunk * step, step)],
            send.at[dist - 1, chunk], recv.at[dist - 1, chunk], {"band": target},
        )

    def edge_hops(way, dist):
        other, target, slots, send, recv = way[1], way[5], way[7], way[8], way[9]
        return [
            remote(
                psi.at[other + at * hy] if dist == 1 else slots.at[dist - 2, at],
                slots.at[dist - 1, at], send.at[dist - 1, at], recv.at[dist - 1, at], {"band": target},
            )
            for at in range(cx)
        ]

    def sends(way, dist):
        place = way[6]
        go = (place >= dist - 1) & (place < lines - 1)
        if ends and dist == 1:
            go = go & (place != lines - 2)
        return go

    def sends_extra(way):
        return way[6] == 0

    def receives_edges(way, dist):
        place = way[6]
        got = place >= dist
        if ends and dist == 1:
            got = got & (place != lines - 1)
        return got

    def receives(way, dist):
        place = way[6]
        got = receives_edges(way, dist)
        if ends and dist == 2:
            got = got | (place == 1)
        return got

    outer = sorted({0, cx - 1, cx, segs - 1})
    order = outer + [at for at in range(segs) if at not in outer]
    for copy in halos:
        copy.start()
    for chunk in range(chunks):
        for way in ways:
            @pl.when(sends(way, 1))
            def _(way=way, chunk=chunk):
                hop(way, 1, chunk).start()
    for way in ways:
        @pl.when(sends(way, 1))
        def _(way=way):
            for copy in edge_hops(way, 1):
                copy.start()
    for at in order:
        swaps[at].start()
    if ends:
        for chunk in range(chunks):
            for way in ways:
                @pl.when(sends_extra(way))
                def _(way=way, chunk=chunk):
                    hop(way, 2, chunk, True).start()

    def left_operand(src, edges, first):
        for at in range(segs):
            h, plane = at // cx, at % cx
            opposite = (1 - h) * half + plane * hy

            def body(y, carry, at=at, h=h, plane=plane, opposite=opposite):
                r = at * hy + y
                here = src[r]
                before = edges[0, h, y] if plane == 0 else src[r - hy]
                after = edges[1, h, y] if plane == cx - 1 else src[r + hy]
                beside = before + after
                beside = beside + src[jnp.where(y == 0, opposite + hy - 1, r - 1)]
                beside = beside + src[jnp.where(y == hy - 1, opposite, r + 1)]
                beside = beside + pltpu.roll(here, 1, 1) + pltpu.roll(here, nz - 1, 1)
                hpsi = 0.5 * (6.0 * here - beside) + pot[r] * here
                for slot, value in ((first, hpsi), (first + 1, here)):
                    high, low = parts(value)
                    lhs_high[r, pl.ds(slot * bands, bands)] = high
                    lhs_low[r, pl.ds(slot * bands, bands)] = low
                return carry

            lax.fori_loop(0, hy, body, 0)

    def accumulate(group, source, lhs_row, right_row, count):
        where = pl.ds(group * 2 * bands, 2 * bands)

        def body(k, carry):
            left, right = [], []
            for pos in range(2):
                r = lhs_row + 2 * k + pos
                high, low = lhs_high[r, where], lhs_low[r, where]
                other_high, other_low = parts(right_row(2 * k + pos))
                left += [high, high, low]
                right += [other_high, other_low, other_high]
            out[source, where] += lax.dot_general(
                jnp.concatenate(left, axis=1), jnp.concatenate(right, axis=1), CONTRACT_LAST,
                preferred_element_type=jnp.float32,
            )
            return carry

        lax.fori_loop(0, count // 2, body, 0)

    def moved(way, dist, chunk, group):
        base, other, slots, place = way[0], way[1], way[2], way[6]
        rows_at = base
        if ends and dist == 2:
            rows_at = jnp.where(place == 1, other, base)
        accumulate(
            group, source_of(way, dist), rows_at + chunk * step,
            lambda r: slots[dist - 1, chunk * step + r], step,
        )

    def three(left, right):
        left_high, left_low = left
        right_high, right_low = right
        return lax.dot_general(
            jnp.concatenate([left_high, left_high, left_low], axis=1),
            jnp.concatenate([right_high, right_low, right_high], axis=1),
            CONTRACT_LAST, preferred_element_type=jnp.float32,
        )

    def source_of(way, dist):
        from_place = jnp.maximum(way[6] - dist, 0)
        return from_place if way is ways[0] else lines - 1 - from_place

    def fix_edges(way, dist, group):
        base, other, slots, edges = way[0], way[1], way[2], way[7]
        source = source_of(way, dist)
        where = pl.ds((2 * group + 1) * bands, bands)
        into = pl.ds(2 * group * bands, bands)
        for at in range(cx):
            across = other + at * hy + hy - 1
            last = base + at * hy + hy - 1
            out[source, into] += 0.5 * (
                three((lhs_high[across, where], lhs_low[across, where]), parts(slots[dist - 1, at * hy]))
                - three((lhs_high[last, where], lhs_low[last, where]), parts(edges[dist - 1, at]))
            )

    def corrects(way, dist):
        go = receives_edges(way, dist)
        if ends:
            go = go & (way[6] != 1)
        return go

    def project(source, group, right):
        for kind in range(2):
            coupled = lax.dot_general(
                coef[group], sym[kind], (((1,), (0,)), ((), ())),
                precision=lax.Precision.HIGHEST, preferred_element_type=jnp.float32,
            )
            out[source, pl.ds((2 * group + kind) * bands, bands)] += three(parts(coupled), parts(right))

    out[...] = jnp.zeros_like(out)
    coef[0] = jnp.zeros_like(coef[0])
    for copy in halos:
        copy.wait_recv()
    left_operand(psi, halo, 0)

    def coef_body(r, carry):
        own = pl.ds(bands, bands)
        coef[0] += three((lhs_high[r, own], lhs_low[r, own]), parts(proj[r]))
        return carry

    lax.fori_loop(0, rows, coef_body, 0)
    accumulate(0, line, 0, lambda r: psi[r], rows)
    project(line, 0, coef[0])
    coef_swap.start()

    @pl.when(line < lines - 1)
    def _():
        coef_hop(1).start()

    for dist in range(1, lines):
        for chunk in range(chunks):
            for way in ways:
                @pl.when(receives(way, dist))
                def _(way=way, dist=dist, chunk=chunk):
                    hop(way, dist, chunk).wait_recv()

                if dist < lines - 1:
                    @pl.when(sends(way, dist + 1))
                    def _(way=way, dist=dist, chunk=chunk):
                        hop(way, dist + 1, chunk).start()
            for way in ways:
                @pl.when(receives(way, dist))
                def _(way=way, dist=dist, chunk=chunk):
                    moved(way, dist, chunk, 0)
        for way in ways:
            @pl.when(receives_edges(way, dist))
            def _(way=way, dist=dist):
                for copy in edge_hops(way, dist):
                    copy.wait_recv()

            if dist < lines - 1:
                @pl.when(sends(way, dist + 1))
                def _(way=way, dist=dist):
                    for copy in edge_hops(way, dist + 1):
                        copy.start()

            @pl.when(corrects(way, dist))
            def _(way=way, dist=dist):
                fix_edges(way, dist, 0)

        @pl.when(line >= dist)
        def _(dist=dist):
            coef_hop(dist).wait_recv()

        if dist < lines - 1:
            @pl.when((line >= dist) & (line < lines - 1))
            def _(dist=dist):
                coef_hop(dist + 1).start()

        @pl.when(line >= dist)
        def _(dist=dist):
            project(line - dist, 0, coef_below[dist - 1])

        if dist == 1:
            for at in outer:
                swaps[at].wait_recv()
            for copy in forwards:
                copy.start()
    for at in range(segs):
        if at not in outer:
            swaps[at].wait_recv()
    coef_swap.wait_recv()
    for copy in forwards:
        copy.wait_recv()
    left_operand(partner, partner_halo, 2)
    accumulate(1, line, 0, lambda r: psi[r], rows)
    project(line, 1, coef[0])
    for dist in range(1, lines):
        for way in ways:
            @pl.when(receives(way, dist))
            def _(way=way, dist=dist):
                for chunk in range(chunks):
                    moved(way, dist, chunk, 1)

            @pl.when(corrects(way, dist))
            def _(way=way, dist=dist):
                fix_edges(way, dist, 1)

        @pl.when(line >= dist)
        def _(dist=dist):
            project(line - dist, 1, coef_below[dist - 1])

    for copy in swaps + halos + forwards + [coef_swap]:
        copy.wait_send()
    for dist in range(1, lines):
        @pl.when((line >= dist - 1) & (line < lines - 1))
        def _(dist=dist):
            coef_hop(dist).wait_send()

        for way in ways:
            @pl.when(sends(way, dist))
            def _(way=way, dist=dist):
                for copy in edge_hops(way, dist):
                    copy.wait_send()

        for chunk in range(chunks):
            for way in ways:
                go = sends(way, dist)
                if ends and dist == 2:
                    go = go | sends_extra(way)

                @pl.when(go)
                def _(way=way, dist=dist, chunk=chunk):
                    hop(way, dist, chunk).wait_send()


def gram(psi, pot, proj, sym, lines, doms, cx, ny):
    rows, bands, nz = psi.shape
    half = rows // 2
    chunks = 4 if half % 8 == 0 else 1
    hops = lines - 1
    dma = pltpu.SemaphoreType.DMA
    vmem = pl.BlockSpec(memory_space=pltpu.VMEM)
    return pl.pallas_call(
        functools.partial(gram_kernel, lines, doms, cx, ny, chunks),
        out_shape=jax.ShapeDtypeStruct((lines, 4 * bands, bands), jnp.float32),
        in_specs=[vmem] * 4,
        out_specs=vmem,
        scratch_shapes=[
            pltpu.VMEM((rows, bands, nz), jnp.float32),
            pltpu.VMEM((2, 2, ny // 2, bands, nz), jnp.float32),
            pltpu.VMEM((2, 2, ny // 2, bands, nz), jnp.float32),
            pltpu.VMEM((hops, half, bands, nz), jnp.float32),
            pltpu.VMEM((hops, half, bands, nz), jnp.float32),
            pltpu.VMEM((rows, 4 * bands, nz), jnp.bfloat16),
            pltpu.VMEM((rows, 4 * bands, nz), jnp.bfloat16),
            pltpu.VMEM((hops, cx, bands, nz), jnp.float32),
            pltpu.VMEM((hops, cx, bands, nz), jnp.float32),
            pltpu.VMEM((2, bands, proj.shape[1]), jnp.float32),
            pltpu.VMEM((hops, bands, proj.shape[1]), jnp.float32),
            dma((2 * cx,)), dma((2 * cx,)), dma((2, 2)), dma((2, 2)), dma((2, 2)), dma((2, 2)),
            dma((hops, chunks)), dma((hops, chunks)), dma((hops, chunks)), dma((hops, chunks)),
            dma((hops, cx)), dma((hops, cx)), dma((hops, cx)), dma((hops, cx)),
            dma((hops,)), dma((hops,)), dma((1,)), dma((1,)),
        ],
        compiler_params=pltpu.CompilerParams(
            collective_id=0, has_side_effects=True, vmem_limit_bytes=62 * 1024 * 1024
        ),
    )(psi, pot, proj, sym)


def on_device(
    wavefunctions, potential, projectors, hamiltonian_correction, delta_s, projector_count
):
    bands, cx, ny, nz = wavefunctions.shape
    groups = lax.axis_size("band")
    doms = lax.axis_size("dom")
    lines = groups // 2
    mine = lax.axis_index("band")
    line, side = mine // 2, mine % 2
    rows = cx * ny
    volume = 1.0 / (rows * nz * doms)
    hy = ny // 2
    psi = jnp.transpose(wavefunctions.reshape(bands, cx, 2, hy, nz), (2, 1, 3, 0, 4)).reshape(rows, bands, nz)
    pot = jnp.transpose(potential.reshape(cx, 2, hy, nz), (1, 0, 2, 3)).reshape(rows, 1, nz)

    atoms, slots = hamiltonian_correction.shape[:2]
    used = atoms * slots
    width = -(-used // 128) * 128
    mask = (jnp.arange(slots, dtype=jnp.int32)[None, :] < projector_count[:, None]).astype(jnp.float32)
    proj = jnp.transpose(projectors.reshape(used, cx, 2, hy, nz), (2, 1, 3, 0, 4)).reshape(rows, used, nz)
    proj = jnp.pad(proj * mask.reshape(1, used, 1), ((0, 0), (0, width - used), (0, 0)))
    sym = (0.5 / volume) * jnp.stack(
        [
            hamiltonian_correction + jnp.swapaxes(hamiltonian_correction, 1, 2),
            delta_s + jnp.swapaxes(delta_s, 1, 2),
        ]
    )
    same_atom = jnp.eye(atoms, dtype=jnp.float32)[None, :, None, :, None]
    sym = (sym[:, :, :, None, :] * same_atom).reshape(2, used, used)
    sym = jnp.pad(sym, ((0, 0), (0, width - used), (0, width - used)))

    grid = gram(psi, pot, proj, sym, lines, doms, cx, ny)
    here = (jnp.arange(lines, dtype=jnp.int32) == line)[:, None, None, None]
    both = grid.reshape(lines, 4, bands, bands)

    split = 4 % doms == 0
    if split:
        both = lax.all_to_all(both[None], "dom", 2, 0, tiled=True).sum(0)
        first = lax.axis_index("dom") * (4 // doms)
    else:
        both = lax.psum(both, "dom")
        first = 0
    count = both.shape[1]
    lanes = [[at * 2 + s for at in range(lines)] for s in range(2)]
    mirrored = lax.all_to_all(both, "band", 0, 0, axis_index_groups=lanes, tiled=True)
    swapped = lax.ppermute(both, "band", [(i, i ^ 1) for i in range(groups)])
    crossed = ((first + jnp.arange(count, dtype=jnp.int32)) >= 2)[None, :, None, None]
    total = volume * jnp.where(crossed, swapped, both) + volume * jnp.where(here, 0.0, jnp.swapaxes(mirrored, 2, 3))
    if split:
        total = lax.all_gather(total, "dom", axis=1, tiled=True)
    total = total.reshape(lines, 2, 2, bands, bands)
    by_side = jnp.where(side == 0, total, total[:, ::-1])
    final = jnp.transpose(by_side, (2, 3, 0, 1, 4)).reshape(2, bands, groups * bands)
    return final[0], final[1]


def solution(mesh):
    placed = (
        P("band", "dom", None, None),
        P("dom", None, None),
        P("dom", None, None, None, None),
        P("dom", None, None),
        P("dom", None, None),
        P("dom"),
    )
    return jax.shard_map(
        on_device,
        mesh=mesh,
        in_specs=placed,
        out_specs=(P("band", None), P("band", None)),
        check_vma=False,
    )
```
